32 devices in a mesh: layer: 2 (over x), row: 4 (over z), col: 4 (over y, core).
Axes of the slice: x: 2, y: 2, z: 4, core: 2. Of those that a mesh axis runs over, the one named last changes fastest.
Arguments:
- left_matrix: float32 [2, 1024, 16384], P(None, 'row', 'col'), may hold values from -6 to 6
- right_matrix: float32 [2, 16384, 512], P(None, 'row', 'col'), may hold values from -0.03125 to 0.03125
Outputs:
- product: float32 [2, 1024, 512], P(None, 'row', 'col')
The draws below stay inside these ranges and needn't reach their ends.
All inputs are finite; a program needn't handle non-finite values.
Results may differ from the reference program's by a relative error of at most 0.000071.
Values sent between devices are 32-bit elements; how exact they have to be, the bound alone decides.
No kernel may reach another device: no remote copies, remote signals or barrier semaphores. Data moves between devices by JAX's collectives and lax.ppermute only.
A program may use at most 128 MiB of HBM per device.

```python
import jax
import jax.numpy as jnp
from jax import lax

K = 16384
M = 1024
NC = 512


def block_scale(key, dims, cuts, smallest, largest):
    gain, own = 1.0, jax.random.fold_in(key, 6)
    for axis_at, shards_of in cuts:
        draws = jnp.exp(jax.random.uniform(jax.random.fold_in(own, axis_at), (shards_of,), jnp.float32, smallest / len(cuts), largest / len(cuts)))
        gain = gain * jnp.repeat(draws, dims[axis_at] // shards_of).reshape([-1 if axis == axis_at else 1 for axis in range(len(dims))])
    return gain


def gaussian(own_key, dims, width, most, cuts=(), kind=jnp.bfloat16):
    entries = width * jax.random.normal(own_key, dims, jnp.float32)
    if cuts:
        entries = entries * block_scale(own_key, dims, cuts, -0.22, 0.18)
    return jnp.clip(entries, -most, most).astype(kind)


def setup_inputs(seed: int = 0) -> dict:
    splits = jax.random.split(jax.random.key(seed), 3)
    left_matrix = gaussian(splits[0], (2, M, K), 1.0, 6.0, ((1, 4), (2, 4)), jnp.float32)
    right_matrix = gaussian(splits[1], (2, K, NC), (2 * K) ** -0.5, 0.03125, ((1, 4), (2, 4)), jnp.float32)
    return dict(left_matrix=left_matrix, right_matrix=right_matrix)


def reference(left_matrix, right_matrix):
    highest = lax.Precision.HIGHEST
    left_real = left_matrix[0]
    left_imag = left_matrix[1]
    right_real = right_matrix[0]
    right_imag = right_matrix[1]
    first_term = jnp.dot(left_real, right_real, precision=highest, preferred_element_type=jnp.float32)
    second_term = jnp.dot(left_imag, right_imag, precision=highest, preferred_element_type=jnp.float32)
    third_term = jnp.dot(left_real + left_imag, right_real + right_imag, precision=highest, preferred_element_type=jnp.float32)
    return jnp.stack([first_term - second_term, third_term - first_term - second_term])
```

```python
import functools

import jax
import jax.numpy as jnp
from jax import lax
from jax.experimental import pallas as pl
from jax.experimental.pallas import tpu as pltpu
from jax.sharding import PartitionSpec as P

LANES = 128
SLAB_PARTS = (4, 4, 4, 4)


def slab_widths(width):
    if width % LANES:
        return [width]
    tiles, total = width // LANES, sum(SLAB_PARTS)
    cuts = sorted({round(tiles * sum(SLAB_PARTS[: i + 1]) / total) for i in range(len(SLAB_PARTS))} | {0})
    return [LANES * (b - a) for a, b in zip(cuts, cuts[1:])]


def parts_of(value):
    high = value.astype(jnp.bfloat16)
    rest = value - high.astype(jnp.float32)
    middle = rest.astype(jnp.bfloat16)
    low = (rest - middle.astype(jnp.float32)).astype(jnp.bfloat16)
    return high, middle, low


def exact_dot(left, right):
    dot = functools.partial(jnp.dot, preferred_element_type=jnp.float32)
    left_high, left_middle, left_low = parts_of(left)
    right_high, right_middle, right_low = parts_of(right)
    small = dot(left_high, right_low) + dot(left_middle, right_middle) + dot(left_low, right_high)
    return dot(left_high, right_high) + (dot(left_high, right_middle) + dot(left_middle, right_high) + small)


def fold_kernel(plan, *refs):
    rows, cols, group, left_from, right_from = plan
    left_refs = refs[: len(left_from)]
    right_refs = refs[len(left_from) : len(left_from) + len(right_from)]
    sum_in, sum_out, left_held, right_held, left_sem, right_sem = refs[len(left_from) + len(right_from) :]
    row_at, col_at = lax.axis_index("row"), lax.axis_index("col")

    for source, ref in zip(left_from, left_refs):
        slot = source(col_at)
        pltpu.make_async_copy(ref, left_held.at[slot], left_sem.at[slot]).start()
    for distance, ref in zip(right_from, right_refs):
        plane = row_at + distance

        @pl.when((plane >= 0) & (plane < rows))
        def _(plane=plane, ref=ref):
            pltpu.make_async_copy(ref, right_held.at[plane], right_sem.at[plane]).start()

    real, imag = sum_in[0], sum_in[1]
    cols_out = real.shape[1]
    total = jnp.concatenate([real, imag], axis=1)
    for plane in range(rows):
        pltpu.make_async_copy(right_refs[0], right_held.at[plane], right_sem.at[plane]).wait()
        for member in range(group):
            slot = plane * group + member
            pltpu.make_async_copy(left_refs[0], left_held.at[slot], left_sem.at[slot]).wait()
            left = jnp.concatenate([left_held[slot, 0], left_held[slot, 1]], axis=1)
            right_real, right_imag = right_held[plane, 0, member], right_held[plane, 1, member]
            right = jnp.concatenate(
                [
                    jnp.concatenate([right_real, right_imag], axis=1),
                    jnp.concatenate([-right_imag, right_real], axis=1),
                ],
                axis=0,
            )
            total = total + exact_dot(left, right)
    sum_out[0] = total[:, :cols_out]
    sum_out[1] = total[:, cols_out:]


def fold(rows, cols, group, left_from, right_from, lefts, rights, total):
    plan = (rows, cols, group, left_from, right_from)
    hbm = pl.BlockSpec(memory_space=pl.ANY)
    vmem = pl.BlockSpec(memory_space=pltpu.VMEM)
    return pl.pallas_call(
        functools.partial(fold_kernel, plan),
        out_shape=jax.ShapeDtypeStruct(total.shape, total.dtype),
        in_specs=[hbm] * (len(lefts) + len(rights)) + [vmem],
        out_specs=vmem,
        scratch_shapes=[
            pltpu.VMEM((cols,) + lefts[0].shape, jnp.float32),
            pltpu.VMEM((rows,) + rights[0].shape, jnp.float32),
            pltpu.SemaphoreType.DMA((cols,)),
            pltpu.SemaphoreType.DMA((rows,)),
        ],
    )(*lefts, *rights, total)


def local(left_matrix, right_matrix):
    layers, rows, cols = (lax.axis_size(name) for name in ("layer", "row", "col"))
    layer_index = lax.axis_index("layer")
    _, local_rows, left_width = left_matrix.shape
    _, right_height, local_cols = right_matrix.shape
    share = left_width // layers
    group = right_height // left_width
    right_view = right_matrix.reshape(2, group, left_width, local_cols)
    cores = 2 if cols % 2 == 0 else 1
    chips = cols // cores

    next_chip = [(c, (c + cores) % cols) for c in range(cols)]
    sibling = [(c, c ^ 1) for c in range(cols)]

    widths = slab_widths(share)
    starts = [sum(widths[:j]) for j in range(len(widths))]
    lefts = [[] for _ in widths]
    rights = [[] for _ in widths]
    for j, (start, width) in enumerate(zip(starts, widths)):
        at = layer_index * share + start
        rights[j].append(lax.dynamic_slice_in_dim(right_view, at, width, 2))
        lefts[j].append(lax.dynamic_slice_in_dim(left_matrix, at, width, 2))
    left_from = []
    for hop in range(chips):
        left_from.append(lambda c, hop=hop: lax.rem(c - hop * cores + cols, cols))
        if cores == 2:
            left_from.append(lambda c, hop=hop: lax.rem(c + 1 - 2 * lax.rem(c, 2) - hop * cores + cols, cols))
    for j in range(len(widths)):
        piece = lefts[j][0]
        lefts[j] = []
        for hop in range(chips):
            if hop:
                piece = lax.ppermute(piece, "col", next_chip)
            lefts[j].append(piece)
            if cores == 2:
                lefts[j].append(lax.ppermute(piece, "col", sibling))
    right_from = [0]
    for hop in range(1, rows):
        right_from += [-hop, hop]
    for j in range(len(widths)):
        up = down = rights[j][0]
        for hop in range(1, rows):
            up = lax.ppermute(up, "row", [(z, z + 1) for z in range(hop - 1, rows - 1)])
            down = lax.ppermute(down, "row", [(z, z - 1) for z in range(1, rows - hop + 1)])
            rights[j] += [up, down]

    total = jnp.zeros((2, local_rows, local_cols), jnp.float32)
    for j in range(len(widths)):
        total = fold(rows, cols, group, left_from, right_from, lefts[j], rights[j], total)
    product = passed = total
    for hop in range(1, layers):
        passed = lax.ppermute(passed, "layer", [(x, (x + 1) % layers) for x in range(layers)])
        product = product + passed
    return product


def solution(mesh):
    in_specs = (P(None, "row", "col"), P(None, "row", "col"))
    out_specs = P(None, "row", "col")
    return jax.shard_map(local, mesh=mesh, in_specs=in_specs, out_specs=out_specs, check_vma=False)
```

```python
import functools

import jax
import jax.numpy as jnp
from jax import lax
from jax.experimental import pallas as pl
from jax.experimental.pallas import tpu as pltpu
from jax.sharding import PartitionSpec as P


LANES = 128
AHEAD = 4
SLAB_PARTS = (5, 5, 3, 3)
SEQUENCE = (
    "cut_0", "r1_0", "r2_1", "yex_0", "sib_0", "r1_1", "r2_0", "r1_2", "r5_1", "r2_2", "cut_1", "sib_1", "yex_1",
    "yex_2", "axf_3", "r4_1", "oth_0", "axf_1", "yex_3", "sib_3", "sib_2", "r4_2", "r5_0", "r2_3", "r1_3", "axf_0",
    "r5_2", "r7_1", "axs_3", "axf_2", "oth_1", "r4_0", "fold_0", "r5_3", "axs_1", "r4_3", "r7_2", "oth_2", "axs_0",
    "fold_2", "axs_2", "r7_3", "oth_3", "fold_1", "extra_0", "fold_3", "fold_4", "extra_1",
)
FOLDS = (
    ("early_0", "early_1"),
    ("outer_0", "outer_1", "outer_2", "outer_3"),
    ("early_2", "late_0", "late_1"),
    ("early_3", "late_2"),
    ("late_3",),
)
READS = dict(early=("own", "r1", "r2", "r5"), late=("r4", "r7"), outer=("own", "r4"))


def slab_widths(width, parts):
    tiles, total = width // LANES, sum(parts)
    if width % LANES or tiles < len(parts):
        return [width]
    cuts = sorted({round(tiles * sum(parts[: i + 1]) / total) for i in range(len(parts))} | {0})
    return [LANES * (b - a) for a, b in zip(cuts, cuts[1:])]


def close_dot(left, right):
    dot = functools.partial(jnp.dot, preferred_element_type=jnp.float32)
    left_high, right_high = left.astype(jnp.bfloat16), right.astype(jnp.bfloat16)
    left_low = (left - left_high.astype(jnp.float32)).astype(jnp.bfloat16)
    right_low = (right - right_high.astype(jnp.float32)).astype(jnp.bfloat16)
    return dot(left_high, right_high) + (dot(left_high, right_low) + dot(left_low, right_high))


def add_product(sum_ref, left, right):
    cols = right.shape[2]
    wide_left = jnp.concatenate([left[0], left[1]], axis=1)
    wide_right = jnp.concatenate(
        [
            jnp.concatenate([right[0], right[1]], axis=1),
            jnp.concatenate([-right[1], right[0]], axis=1),
        ],
        axis=0,
    )
    both = close_dot(wide_left, wide_right)
    sum_ref[0] += both[:, :cols]
    sum_ref[1] += both[:, cols:]


def call_kernel(kernel, operands, totals, scratch_shapes):
    hbm = pl.BlockSpec(memory_space=pl.ANY)
    vmem = pl.BlockSpec(memory_space=pltpu.VMEM)
    out = [jax.ShapeDtypeStruct(total.shape, total.dtype) for total in totals]
    return pl.pallas_call(
        kernel,
        out_shape=out,
        in_specs=[hbm] * len(operands) + [vmem] * len(totals),
        out_specs=[vmem] * len(totals),
        scratch_shapes=scratch_shapes,
    )(*operands, *totals)


def chain_kernel(rows, group, left_from, right_from, *refs):
    left_refs = refs[: len(left_from)]
    right_refs = refs[len(left_from) : len(left_from) + len(right_from)]
    sum_in, sum_out, left_held, right_held, left_sem, right_sem = refs[len(left_from) + len(right_from) :]
    row_at, col_at = lax.axis_index("row"), lax.axis_index("col")
    for source, ref in zip(left_from, left_refs):
        slot = source(col_at)
        pltpu.make_async_copy(ref, left_held.at[slot], left_sem.at[slot]).start()
    for distance, ref in zip(right_from, right_refs):
        plane = row_at + distance

        @pl.when((plane >= 0) & (plane < rows))
        def _(plane=plane, ref=ref):
            pltpu.make_async_copy(ref, right_held.at[plane], right_sem.at[plane]).start()

    sum_out[...] = sum_in[...]

    @pl.loop(0, rows)
    def _(plane):
        pltpu.make_async_copy(right_refs[0], right_held.at[plane], right_sem.at[plane]).wait()
        for member in range(group):
            slot = plane * group + member
            pltpu.make_async_copy(left_refs[0], left_held.at[slot], left_sem.at[slot]).wait()
            add_product(sum_out, left_held[slot], right_held[plane, :, member])


def gather_chain(left_matrix, right_matrix):
    layers, rows, cols = (lax.axis_size(name) for name in ("layer", "row", "col"))
    layer_index = lax.axis_index("layer")
    _, local_rows, left_width = left_matrix.shape
    _, right_height, local_cols = right_matrix.shape
    share = left_width // layers
    group = right_height // left_width
    right_view = right_matrix.reshape(2, group, left_width, local_cols)
    cores = 2 if cols % 2 == 0 else 1
    next_chip = [(c, (c + cores) % cols) for c in range(cols)]
    sibling = [(c, c ^ 1) for c in range(cols)]
    left_from, right_from = [], [0]
    for hop in range(cols // cores):
        left_from.append(lambda c, hop=hop: lax.rem(c - hop * cores + cols, cols))
        if cores == 2:
            left_from.append(lambda c, hop=hop: lax.rem(c + 1 - 2 * lax.rem(c, 2) - hop * cores + cols, cols))
    for hop in range(1, rows):
        right_from += [-hop, hop]
    total, start = jnp.zeros((2, local_rows, local_cols), jnp.float32), 0
    for width in slab_widths(share, (1, 1)):
        at = layer_index * share + start
        start += width
        own = lax.dynamic_slice_in_dim(right_view, at, width, 2)
        rights, up, down = [own], own, own
        for hop in range(1, rows):
            up = lax.ppermute(up, "row", [(z, z + 1) for z in range(hop - 1, rows - 1)])
            down = lax.ppermute(down, "row", [(z, z - 1) for z in range(1, rows - hop + 1)])
            rights += [up, down]
        piece, lefts = lax.dynamic_slice_in_dim(left_matrix, at, width, 2), []
        for hop in range(cols // cores):
            if hop:
                piece = lax.ppermute(piece, "col", next_chip)
            lefts.append(piece)
            if cores == 2:
                lefts.append(lax.ppermute(piece, "col", sibling))
        scratch = [
            pltpu.VMEM((cols,) + lefts[0].shape, jnp.float32),
            pltpu.VMEM((rows,) + own.shape, jnp.float32),
            pltpu.SemaphoreType.DMA((cols,)),
            pltpu.SemaphoreType.DMA((rows,)),
        ]
        kernel = functools.partial(chain_kernel, rows, group, left_from, right_from)
        (total,) = call_kernel(kernel, lefts + rights, [total], scratch)
    product = passed = total
    for _ in range(1, layers):
        passed = lax.ppermute(passed, "layer", [(x, (x + 1) % layers) for x in range(layers)])
        product = product + passed
    return product


def own_place(plane, col):
    return plane + (3 - 2 * plane) * (col // 2)


def line_pairs(moves, only=lambda place, chip_col: True):
    pairs = []
    for chip_col in range(4):
        for place, target in moves:
            if only(place, chip_col):
                flip = 3 if chip_col >= 2 else 0
                pairs.append((4 * (place ^ flip) + chip_col, 4 * (target ^ flip) + chip_col))
    return pairs


def owns_left_out(place, chip_col):
    counted = chip_col ^ (3 if chip_col >= 2 else 0)
    return counted == (1 if place == 0 else 0)


def sources(kind, first, last):
    every = dict(
        own={0: 0, 1: 1, 2: 2, 3: 3},
        r1={1: 0, 2: 3, 3: 2} | ({0: 1} if first else {}),
        r2={1: 2, 2: 1},
        r4={1: 3, 2: 0},
        r5={0: 2, 3: 1},
        r7=({} if first else {0: 3}) | ({3: 0} if last else {}),
    )
    if kind == "outer":
        every = dict(own={} if first else {1: 1}, r4=({1: 3} if first else {}) | ({} if last else {2: 0}))
    return {key: every[key] for key in READS[kind] if every[key]}


def keys_of(kind, first, last):
    lefts = ["axf", "axs"] if kind == "outer" else ["own", "sib", "yex", "oth"]
    return lefts + ["right_" + key for key in sources(kind, first, last)]


def is_one_of(value, options):
    return functools.reduce(jnp.logical_or, [value == option for option in options])


def pick(place, table):
    return sum(jnp.where(place == key, value, 0) for key, value in table.items())


def line_kernel(tasks, sums, extras, *refs):
    plane, col = lax.axis_index("row"), lax.axis_index("col")
    flip = col // 2
    place = own_place(plane, col)
    counted = col + (3 - 2 * col) * flip
    core, chip = lax.rem(counted, 2), counted // 2
    owner = core == jnp.where(place == 1, 1, 0)
    slots = dict(own=2 * chip + core, sib=2 * chip + 1 - core, yex=2 - 2 * chip + core, oth=3 - 2 * chip - core)

    refs = list(refs)
    task_refs = [{key: refs.pop(0) for key in keys_of(*task)} for task in tasks]
    parts_in = [[refs.pop(0) for _ in range(max(count - 1, 0))] for count in (sums, extras)]
    outs = [refs.pop(0) if count else None for count in (sums, extras)]
    scratch = [[refs.pop(0) for _ in range(4)] for _ in tasks]
    total_sem = refs[0]

    def fetch(condition, source, ref, sem):
        @pl.when(condition)
        def _():
            pltpu.make_async_copy(source, ref, sem).start()

    steps = []
    for task, source, (left_held, right_held, left_sem, right_sem) in zip(tasks, task_refs, scratch):
        kind, table = task[0], sources(*task)
        pairs = [4 * p + piece for where in table.values() for p, piece in where.items()]
        needed = is_one_of(place, [pair // 4 for pair in pairs])
        many = kind == "early"
        for key, where in table.items():
            slot = pick(place, where)
            right, sem = (right_held.at[slot], right_sem.at[slot]) if many else (right_held, right_sem)
            fetch(is_one_of(place, where), source["right_" + key], right, sem)
        if many:
            for i, (key, slot) in enumerate(slots.items()):
                wanted = is_one_of(4 * place + slot, pairs)
                left = (left_held.at[i], left_sem.at[i])
                steps.append((wanted, [(wanted, source[key])], left, (right_held.at[slot], right_sem.at[slot]), outs[0]))
            continue
        if kind == "outer":
            choices = [(needed & owner, source["axf"]), (needed & jnp.logical_not(owner), source["axs"])]
        else:
            choices = [(is_one_of(4 * place + slot, pairs), source[key]) for key, slot in slots.items()]
        out = outs[1] if kind == "outer" else outs[0]
        steps.append((needed, choices, (left_held, left_sem), (right_held, right_sem), out))

    def start(number):
        if number < len(steps):
            _, choices, left, _, _ = steps[number]
            for condition, source in choices:
                fetch(condition, source, *left)

    for number in range(AHEAD):
        start(number)
    reads = []
    for number, (out, parts) in enumerate(zip(outs, parts_in)):
        if parts:
            reads.append(pltpu.make_async_copy(parts[0], out, total_sem.at[number]))
        elif out is not None:
            out[...] = jnp.zeros_like(out)
    for read in reads:
        read.start()
    for read in reads:
        read.wait()

    for number, (wanted, choices, left, right, out) in enumerate(steps):

        @pl.when(wanted)
        def _(choices=choices, left=left, right=right):
            pltpu.make_async_copy(right[0], *right).wait()
            pltpu.make_async_copy(choices[0][1], *left).wait()

        start(number + AHEAD)

        @pl.when(wanted)
        def _(left=left, right=right, out=out):
            add_product(out, left[0][...], right[0][...])


def cut_kernel(pieces, share, *refs):
    count = len(pieces)
    wholes, outs, held, (into, out_of) = refs[:2], refs[2 : 2 + count], refs[2 + count : 2 + 2 * count], refs[2 + 2 * count :]
    copies = []
    for i, (factor, axis, start, width) in enumerate(pieces):
        at = pl.multiple_of(lax.axis_index("layer") * share + start, LANES)
        whole = wholes[factor]
        part = whole.at[:, :, pl.ds(at, width)] if axis == 2 else whole.at[:, pl.ds(at, width)]
        read = pltpu.make_async_copy(part, held[i], into.at[i])
        read.start()
        copies.append((read, pltpu.make_async_copy(held[i], outs[i], out_of.at[i])))
    for read, write in copies:
        read.wait()
        write.start()
    for _, write in copies:
        write.wait()


def cut(factors, pieces, share):
    shapes = []
    for factor, axis, _, width in pieces:
        shape = list(factors[factor].shape)
        shape[axis] = width
        shapes.append(tuple(shape))
    hbm = pl.BlockSpec(memory_space=pl.ANY)
    return pl.pallas_call(
        functools.partial(cut_kernel, pieces, share),
        out_shape=[jax.ShapeDtypeStruct(shape, jnp.float32) for shape in shapes],
        in_specs=[hbm] * 2,
        out_specs=[hbm] * len(pieces),
        scratch_shapes=[pltpu.VMEM(shape, jnp.float32) for shape in shapes] + [pltpu.SemaphoreType.DMA((len(pieces),))] * 2,
        name="cut",
    )(*factors)


def gather_line(left_matrix, right_matrix):
    layers = lax.axis_size("layer")
    _, local_rows, left_width = left_matrix.shape
    local_cols = right_matrix.shape[2]
    share = left_width // layers
    widths = slab_widths(share, SLAB_PARTS)
    final = len(widths) - 1
    grid = ("row", "col")
    across = [(c, c ^ 2) for c in range(4)]
    sibling = [(c, c ^ 1) for c in range(4)]
    held = {}
    total = extra = None
    extras = []
    place = own_place(lax.axis_index("row"), lax.axis_index("col"))

    def fold(number, total, extra):
        tasks, operands, scratch = [], [], []
        for task in FOLDS[number]:
            kind, slab = task.split("_")
            slab = int(slab)
            tasks.append((kind, slab == 0, slab == final))
            left, right = held["left"][slab], held["right"][slab]
            for key in keys_of(*tasks[-1]):
                if key in ("own", "right_own"):
                    operands.append(left if key == "own" else right)
                else:
                    operands.append(held[f"{key.removeprefix('right_')}_{slab}"])
            many = (4,) if kind == "early" else ()
            scratch += [pltpu.VMEM(many + left.shape, jnp.float32), pltpu.VMEM(many + right.shape, jnp.float32)]
            scratch += [pltpu.SemaphoreType.DMA(many)] * 2
        sum_in = [] if total is None else [total]
        extra_in = [] if extra is None else [extra]
        has_sum = any(task[0] != "outer" for task in tasks)
        has_extra = any(task[0] == "outer" for task in tasks)
        sums, extras = has_sum * (1 + len(sum_in)), has_extra * (1 + len(extra_in))
        totals = has_sum * sum_in + has_extra * extra_in
        shape = jax.ShapeDtypeStruct((2, local_rows, local_cols), jnp.float32)
        vmem = pl.BlockSpec(memory_space=pltpu.VMEM)
        out = pl.pallas_call(
            functools.partial(line_kernel, tasks, sums, extras),
            out_shape=[shape] * (has_sum + has_extra),
            in_specs=[pl.BlockSpec(memory_space=pl.ANY)] * len(operands + totals),
            out_specs=[vmem] * (has_sum + has_extra),
            scratch_shapes=scratch + [pltpu.SemaphoreType.DMA((2,))],
        )(*operands, *totals)
        return out[0] if has_sum else total, out[-1] if has_extra else extra

    for name in SEQUENCE:
        step, slab = name.split("_")
        slab = int(slab)
        last = slab == final
        if step in ("fold", "cut"):
            if step == "fold":
                total, extra = fold(slab, total, extra)
            else:
                starts = [sum(widths[:j]) for j in range(len(widths))]
                factors = left_matrix, right_matrix
                rights = [(1, 1, *at) for at in zip(starts, widths)]
                lefts = [(0, 2, *at) for at in zip(starts, widths)]
                if slab == 0:
                    *held["right"], first_left = cut(factors, rights + lefts[:1], share)
                else:
                    held["left"] = [first_left] + list(cut(factors, lefts[1:], share))
            continue
        left = lambda slab=slab: held["left"][slab] if slab else first_left
        right = lambda slab=slab: held["right"][slab]
        get = lambda key, slab=slab: held[f"{key}_{slab}"]
        if step == "yex":
            out = lax.ppermute(left(), "col", across)
        elif step == "sib":
            out = lax.ppermute(left(), "col", sibling)
        elif step == "oth":
            out = lax.ppermute(get("yex"), "col", sibling)
        elif step == "axf":
            piece = jnp.where(place == 0, get("yex"), left()) if slab == 0 else left()
            out = lax.ppermute(piece, grid, line_pairs([(0, 1)] + ([] if last else [(3, 2)]), owns_left_out))
        elif step == "axs":
            out = lax.ppermute(get("axf"), "col", sibling)
        elif step == "r1":
            out = lax.ppermute(right(), grid, line_pairs([(0, 1), (2, 3), (3, 2)] + ([] if slab else [(1, 0)])))
        elif step == "r2":
            out = lax.ppermute(right(), grid, line_pairs([(1, 2), (2, 1)]))
        elif step == "r4":
            out = lax.ppermute(get("r1"), grid, line_pairs([(1, 2), (2, 1)]))
        elif step == "r5":
            out = lax.ppermute(get("r2"), grid, line_pairs([(1, 0), (2, 3)]))
        elif step == "r7":
            out = lax.ppermute(get("r4"), grid, line_pairs([(1, 0)] + ([(2, 3)] if last else [])))
        elif step == "extra":
            pairs = line_pairs([(1, 0), (2, 3)])
            pairs = [(16 * x + a, 16 * ((x + slab) % layers) + b) for x in range(layers) for a, b in pairs]
            out = lax.ppermute(extra, ("layer",) + grid, pairs)
            extras.append(out)
        held[name] = out
    passed = lax.ppermute(total, "layer", [(x, x ^ 1) for x in range(layers)])
    return (total + passed) + (extras[0] + extras[1])


def solution(mesh):
    in_specs = (P(None, "row", "col"), P(None, "row", "col"))
    out_specs = P(None, "row", "col")
    shape = dict(mesh.shape)

    def local(left_matrix, right_matrix):
        layers = shape["layer"]
        share = left_matrix.shape[2] // layers
        square = left_matrix.shape[2] == right_matrix.shape[1] and shape["row"] == shape["col"] == 4
        square = square and layers == 2
        if square and len(slab_widths(share, SLAB_PARTS)) == len(SLAB_PARTS):
            return gather_line(left_matrix, right_matrix)
        return gather_chain(left_matrix, right_matrix)

    step = jax.shard_map(local, mesh=mesh, in_specs=in_specs, out_specs=out_specs, check_vma=False)
    if shape["row"] == shape["col"] == 4 and shape["layer"] == 2:
        return step
    return step
```

```python
import functools

import jax
import jax.numpy as jnp
from jax import lax
from jax.experimental import pallas as pl
from jax.experimental.pallas import tpu as pltpu
from jax.sharding import PartitionSpec as P


LANES = 128
AHEAD = 4
SLAB_PARTS = (4, 5, 4, 3)
SEQUENCE = (
    "cut_0", "r1_0", "r2_0", "yex_0", "cut_1", "r2_1", "r1_1", "r1_2", "yex_1", "r2_2", "sib_1", "sib_2", "r1_3",
    "r5_0", "yex_2", "sib_3", "r5_1", "r4_1", "oth_0", "axf_1", "r2_3", "sib_0", "r4_2", "r4_0", "r5_2", "axf_0",
    "yex_3", "r4_3", "r7_1", "r5_3", "oth_1", "axf_2", "axs_1", "fold_0", "axf_3", "oth_2", "r7_2", "axs_0",
    "axs_2", "fold_2", "axs_3", "r7_3", "oth_3", "fold_1", "extra_0", "extra_1", "fold_3", "fold_4",
)
FOLDS = (
    ("early_0", "early_1"),
    ("outer_0", "outer_1", "outer_2", "outer_3"),
    ("early_2", "late_0", "late_1"),
    ("early_3", "late_2"),
    ("late_3",),
)
READS = dict(early=("own", "r1", "r2", "r5"), late=("r4", "r7"), outer=("own", "r4"))


def slab_widths(width, parts):
    tiles, total = width // LANES, sum(parts)
    if width % LANES or tiles < len(parts):
        return [width]
    cuts = sorted({round(tiles * sum(parts[: i + 1]) / total) for i in range(len(parts))} | {0})
    return [LANES * (b - a) for a, b in zip(cuts, cuts[1:])]


def close_dot(left, right):
    dot = functools.partial(jnp.dot, preferred_element_type=jnp.float32)
    left_high, right_high = left.astype(jnp.bfloat16), right.astype(jnp.bfloat16)
    left_low = (left - left_high.astype(jnp.float32)).astype(jnp.bfloat16)
    right_low = (right - right_high.astype(jnp.float32)).astype(jnp.bfloat16)
    return dot(left_high, right_high) + (dot(left_high, right_low) + dot(left_low, right_high))


def add_product(sum_ref, left, right):
    cols = right.shape[2]
    wide_left = jnp.concatenate([left[0], left[1]], axis=1)
    wide_right = jnp.concatenate(
        [
            jnp.concatenate([right[0], right[1]], axis=1),
            jnp.concatenate([-right[1], right[0]], axis=1),
        ],
        axis=0,
    )
    both = close_dot(wide_left, wide_right)
    sum_ref[0] += both[:, :cols]
    sum_ref[1] += both[:, cols:]


def call_kernel(kernel, operands, totals, scratch_shapes):
    hbm = pl.BlockSpec(memory_space=pl.ANY)
    vmem = pl.BlockSpec(memory_space=pltpu.VMEM)
    out = [jax.ShapeDtypeStruct(total.shape, total.dtype) for total in totals]
    return pl.pallas_call(
        kernel,
        out_shape=out,
        in_specs=[hbm] * len(operands) + [vmem] * len(totals),
        out_specs=[vmem] * len(totals),
        scratch_shapes=scratch_shapes,
    )(*operands, *totals)


def chain_kernel(rows, group, left_from, right_from, *refs):
    left_refs = refs[: len(left_from)]
    right_refs = refs[len(left_from) : len(left_from) + len(right_from)]
    sum_in, sum_out, left_held, right_held, left_sem, right_sem = refs[len(left_from) + len(right_from) :]
    row_at, col_at = lax.axis_index("row"), lax.axis_index("col")
    for source, ref in zip(left_from, left_refs):
        slot = source(col_at)
        pltpu.make_async_copy(ref, left_held.at[slot], left_sem.at[slot]).start()
    for distance, ref in zip(right_from, right_refs):
        plane = row_at + distance

        @pl.when((plane >= 0) & (plane < rows))
        def _(plane=plane, ref=ref):
            pltpu.make_async_copy(ref, right_held.at[plane], right_sem.at[plane]).start()

    sum_out[...] = sum_in[...]

    @pl.loop(0, rows)
    def _(plane):
        pltpu.make_async_copy(right_refs[0], right_held.at[plane], right_sem.at[plane]).wait()
        for member in range(group):
            slot = plane * group + member
            pltpu.make_async_copy(left_refs[0], left_held.at[slot], left_sem.at[slot]).wait()
            add_product(sum_out, left_held[slot], right_held[plane, :, member])


def gather_chain(left_matrix, right_matrix):
    layers, rows, cols = (lax.axis_size(name) for name in ("layer", "row", "col"))
    layer_index = lax.axis_index("layer")
    _, local_rows, left_width = left_matrix.shape
    _, right_height, local_cols = right_matrix.shape
    share = left_width // layers
    group = right_height // left_width
    right_view = right_matrix.reshape(2, group, left_width, local_cols)
    cores = 2 if cols % 2 == 0 else 1
    next_chip = [(c, (c + cores) % cols) for c in range(cols)]
    sibling = [(c, c ^ 1) for c in range(cols)]
    left_from, right_from = [], [0]
    for hop in range(cols // cores):
        left_from.append(lambda c, hop=hop: lax.rem(c - hop * cores + cols, cols))
        if cores == 2:
            left_from.append(lambda c, hop=hop: lax.rem(c + 1 - 2 * lax.rem(c, 2) - hop * cores + cols, cols))
    for hop in range(1, rows):
        right_from += [-hop, hop]
    total, start = jnp.zeros((2, local_rows, local_cols), jnp.float32), 0
    for width in slab_widths(share, (1, 1)):
        at = layer_index * share + start
        start += width
        own = lax.dynamic_slice_in_dim(right_view, at, width, 2)
        rights, up, down = [own], own, own
        for hop in range(1, rows):
            up = lax.ppermute(up, "row", [(z, z + 1) for z in range(hop - 1, rows - 1)])
            down = lax.ppermute(down, "row", [(z, z - 1) for z in range(1, rows - hop + 1)])
            rights += [up, down]
        piece, lefts = lax.dynamic_slice_in_dim(left_matrix, at, width, 2), []
        for hop in range(cols // cores):
            if hop:
                piece = lax.ppermute(piece, "col", next_chip)
            lefts.append(piece)
            if cores == 2:
                lefts.append(lax.ppermute(piece, "col", sibling))
        scratch = [
            pltpu.VMEM((cols,) + lefts[0].shape, jnp.float32),
            pltpu.VMEM((rows,) + own.shape, jnp.float32),
            pltpu.SemaphoreType.DMA((cols,)),
            pltpu.SemaphoreType.DMA((rows,)),
        ]
        kernel = functools.partial(chain_kernel, rows, group, left_from, right_from)
        (total,) = call_kernel(kernel, lefts + rights, [total], scratch)
    product = passed = total
    for _ in range(1, layers):
        passed = lax.ppermute(passed, "layer", [(x, (x + 1) % layers) for x in range(layers)])
        product = product + passed
    return product


def own_place(plane, col):
    return plane + (3 - 2 * plane) * (col // 2)


def line_pairs(moves, only=lambda place, chip_col: True):
    pairs = []
    for chip_col in range(4):
        for place, target in moves:
            if only(place, chip_col):
                flip = 3 if chip_col >= 2 else 0
                pairs.append((4 * (place ^ flip) + chip_col, 4 * (target ^ flip) + chip_col))
    return pairs


def owns_left_out(place, chip_col):
    counted = chip_col ^ (3 if chip_col >= 2 else 0)
    return counted == (1 if place == 0 else 0)


def sources(kind, first, last):
    every = dict(
        own={0: 0, 1: 1, 2: 2, 3: 3},
        r1={1: 0, 2: 3, 3: 2} | ({0: 1} if first else {}),
        r2={1: 2, 2: 1},
        r4={1: 3, 2: 0},
        r5={0: 2, 3: 1},
        r7=({} if first else {0: 3}) | ({3: 0} if last else {}),
    )
    if kind == "outer":
        every = dict(own={} if first else {1: 1}, r4=({1: 3} if first else {}) | ({} if last else {2: 0}))
    return {key: every[key] for key in READS[kind] if every[key]}


def keys_of(kind, first, last):
    lefts = ["axf", "axs"] if kind == "outer" else ["own", "sib", "yex", "oth"]
    return lefts + ["right_" + key for key in sources(kind, first, last)]


def is_one_of(value, options):
    return functools.reduce(jnp.logical_or, [value == option for option in options])


def pick(place, table):
    return sum(jnp.where(place == key, value, 0) for key, value in table.items())


def line_kernel(tasks, sums, extras, *refs):
    plane, col = lax.axis_index("row"), lax.axis_index("col")
    flip = col // 2
    place = own_place(plane, col)
    counted = col + (3 - 2 * col) * flip
    core, chip = lax.rem(counted, 2), counted // 2
    owner = core == jnp.where(place == 1, 1, 0)
    slots = dict(own=2 * chip + core, sib=2 * chip + 1 - core, yex=2 - 2 * chip + core, oth=3 - 2 * chip - core)

    refs = list(refs)
    task_refs = [{key: refs.pop(0) for key in keys_of(*task[:3])} for task in tasks]
    parts_in = [[refs.pop(0) for _ in range(max(count - 1, 0))] for count in (sums, extras)]
    outs = [refs.pop(0) if count else None for count in (sums, extras)]
    scratch = [[refs.pop(0) for _ in range(4)] for _ in tasks]
    total_sem = refs[0]

    def fetch(condition, source, ref, sem):
        @pl.when(condition)
        def _():
            pltpu.make_async_copy(source, ref, sem).start()

    steps = []
    for task, source, (left_held, right_held, left_sem, right_sem) in zip(tasks, task_refs, scratch):
        kind, table, swapped = task[0], sources(*task[:3]), task[3]
        pairs = [4 * p + piece for where in table.values() for p, piece in where.items()]
        needed = is_one_of(place, [pair // 4 for pair in pairs])
        many = kind == "early"
        for key, where in table.items():
            slot = pick(place, where)
            right, sem = (right_held.at[slot], right_sem.at[slot]) if many else (right_held, right_sem)
            fetch(is_one_of(place, where), source["right_" + key], right, sem)
        if many:
            for i, (key, slot) in enumerate(slots.items()):
                wanted = is_one_of(4 * place + slot, pairs)
                left = (left_held.at[i], left_sem.at[i])
                steps.append((wanted, [(wanted, source[key])], left, (right_held.at[slot], right_sem.at[slot]), outs[0]))
            continue
        if kind == "outer":
            direct, passed_on = ("axs", "axf") if swapped else ("axf", "axs")
            choices = [(needed & owner, source[direct]), (needed & jnp.logical_not(owner), source[passed_on])]
        else:
            choices = [(is_one_of(4 * place + slot, pairs), source[key]) for key, slot in slots.items()]
        out = outs[1] if kind == "outer" else outs[0]
        steps.append((needed, choices, (left_held, left_sem), (right_held, right_sem), out))

    def start(number):
        if number < len(steps):
            _, choices, left, _, _ = steps[number]
            for condition, source in choices:
                fetch(condition, source, *left)

    for number in range(AHEAD):
        start(number)
    reads = []
    for number, (out, parts) in enumerate(zip(outs, parts_in)):
        if parts:
            reads.append(pltpu.make_async_copy(parts[0], out, total_sem.at[number]))
        elif out is not None:
            out[...] = jnp.zeros_like(out)
    for read in reads:
        read.start()
    for read in reads:
        read.wait()

    for number, (wanted, choices, left, right, out) in enumerate(steps):

        @pl.when(wanted)
        def _(choices=choices, left=left, right=right):
            pltpu.make_async_copy(right[0], *right).wait()
            pltpu.make_async_copy(choices[0][1], *left).wait()

        start(number + AHEAD)

        @pl.when(wanted)
        def _(left=left, right=right, out=out):
            add_product(out, left[0][...], right[0][...])


def cut_kernel(pieces, share, *refs):
    count = len(pieces)
    wholes, outs, held, (into, out_of) = refs[:2], refs[2 : 2 + count], refs[2 + count : 2 + 2 * count], refs[2 + 2 * count :]
    copies = []
    for i, (factor, axis, start, width) in enumerate(pieces):
        at = pl.multiple_of(lax.axis_index("layer") * share + start, LANES)
        whole = wholes[factor]
        part = whole.at[:, :, pl.ds(at, width)] if axis == 2 else whole.at[:, pl.ds(at, width)]
        read = pltpu.make_async_copy(part, held[i], into.at[i])
        read.start()
        copies.append((read, pltpu.make_async_copy(held[i], outs[i], out_of.at[i])))
    for read, write in copies:
        read.wait()
        write.start()
    for _, write in copies:
        write.wait()


def cut(factors, pieces, share):
    shapes = []
    for factor, axis, _, width in pieces:
        shape = list(factors[factor].shape)
        shape[axis] = width
        shapes.append(tuple(shape))
    hbm = pl.BlockSpec(memory_space=pl.ANY)
    return pl.pallas_call(
        functools.partial(cut_kernel, pieces, share),
        out_shape=[jax.ShapeDtypeStruct(shape, jnp.float32) for shape in shapes],
        in_specs=[hbm] * 2,
        out_specs=[hbm] * len(pieces),
        scratch_shapes=[pltpu.VMEM(shape, jnp.float32) for shape in shapes] + [pltpu.SemaphoreType.DMA((len(pieces),))] * 2,
        name="cut",
    )(*factors)


def gather_line(left_matrix, right_matrix):
    layers = lax.axis_size("layer")
    _, local_rows, left_width = left_matrix.shape
    local_cols = right_matrix.shape[2]
    share = left_width // layers
    widths = slab_widths(share, SLAB_PARTS)
    final = len(widths) - 1
    grid = ("row", "col")
    across = [(c, c ^ 2) for c in range(4)]
    sibling = [(c, c ^ 1) for c in range(4)]
    held = {}
    total = extra = None
    extras = []
    place = own_place(lax.axis_index("row"), lax.axis_index("col"))

    def fold(number, total, extra):
        tasks, operands, scratch = [], [], []
        for task in FOLDS[number]:
            kind, slab = task.split("_")
            slab = int(slab)
            tasks.append((kind, slab == 0, slab == final, slab % 2 == 1))
            left, right = held["left"][slab], held["right"][slab]
            for key in keys_of(*tasks[-1][:3]):
                if key in ("own", "right_own"):
                    operands.append(left if key == "own" else right)
                else:
                    operands.append(held[f"{key.removeprefix('right_')}_{slab}"])
            many = (4,) if kind == "early" else ()
            scratch += [pltpu.VMEM(many + left.shape, jnp.float32), pltpu.VMEM(many + right.shape, jnp.float32)]
            scratch += [pltpu.SemaphoreType.DMA(many)] * 2
        sum_in = [] if total is None else [total]
        extra_in = [] if extra is None else [extra]
        has_sum = any(task[0] != "outer" for task in tasks)
        has_extra = any(task[0] == "outer" for task in tasks)
        sums, extras = has_sum * (1 + len(sum_in)), has_extra * (1 + len(extra_in))
        totals = has_sum * sum_in + has_extra * extra_in
        shape = jax.ShapeDtypeStruct((2, local_rows, local_cols), jnp.float32)
        vmem = pl.BlockSpec(memory_space=pltpu.VMEM)
        out = pl.pallas_call(
            functools.partial(line_kernel, tasks, sums, extras),
            out_shape=[shape] * (has_sum + has_extra),
            in_specs=[pl.BlockSpec(memory_space=pl.ANY)] * len(operands + totals),
            out_specs=[vmem] * (has_sum + has_extra),
            scratch_shapes=scratch + [pltpu.SemaphoreType.DMA((2,))],
        )(*operands, *totals)
        return out[0] if has_sum else total, out[-1] if has_extra else extra

    for name in SEQUENCE:
        step, slab = name.split("_")
        slab = int(slab)
        last = slab == final
        if step in ("fold", "cut"):
            if step == "fold":
                total, extra = fold(slab, total, extra)
            else:
                starts = [sum(widths[:j]) for j in range(len(widths))]
                factors = left_matrix, right_matrix
                rights = [(1, 1, *at) for at in zip(starts, widths)]
                lefts = [(0, 2, *at) for at in zip(starts, widths)]
                if slab == 0:
                    *held["right"], first_left = cut(factors, rights + lefts[:1], share)
                else:
                    held["left"] = [first_left] + list(cut(factors, lefts[1:], share))
            continue
        left = lambda slab=slab: held["left"][slab] if slab else first_left
        right = lambda slab=slab: held["right"][slab]
        get = lambda key, slab=slab: held[f"{key}_{slab}"]
        if step == "yex":
            out = lax.ppermute(left(), "col", across)
        elif step == "sib":
            out = lax.ppermute(left(), "col", sibling)
        elif step == "oth":
            out = lax.ppermute(get("yex"), "col", sibling)
        elif step == "axf":
            piece = jnp.where(place == 0, get("yex"), left()) if slab == 0 else get("sib") if slab % 2 else left()
            sender = (lambda *at: not owns_left_out(*at)) if slab % 2 else owns_left_out
            out = lax.ppermute(piece, grid, line_pairs([(0, 1)] + ([] if last else [(3, 2)]), sender))
        elif step == "axs":
            out = lax.ppermute(get("axf"), "col", sibling)
        elif step == "r1":
            out = lax.ppermute(right(), grid, line_pairs([(0, 1), (2, 3), (3, 2)] + ([] if slab else [(1, 0)])))
        elif step == "r2":
            out = lax.ppermute(right(), grid, line_pairs([(1, 2), (2, 1)]))
        elif step == "r4":
            out = lax.ppermute(get("r1"), grid, line_pairs([(1, 2), (2, 1)]))
        elif step == "r5":
            out = lax.ppermute(get("r2"), grid, line_pairs([(1, 0), (2, 3)]))
        elif step == "r7":
            out = lax.ppermute(get("r4"), grid, line_pairs([(1, 0)] + ([(2, 3)] if last else [])))
        elif step == "extra":
            pairs = line_pairs([(1, 0), (2, 3)])
            pairs = [(16 * x + a, 16 * ((x + slab) % layers) + b) for x in range(layers) for a, b in pairs]
            out = lax.ppermute(extra, ("layer",) + grid, pairs)
            extras.append(out)
        held[name] = out
    passed = lax.ppermute(total, "layer", [(x, x ^ 1) for x in range(layers)])
    return (total + passed) + (extras[0] + extras[1])


def solution(mesh):
    in_specs = (P(None, "row", "col"), P(None, "row", "col"))
    out_specs = P(None, "row", "col")
    shape = dict(mesh.shape)

    def local(left_matrix, right_matrix):
        layers = shape["layer"]
        share = left_matrix.shape[2] // layers
        square = left_matrix.shape[2] == right_matrix.shape[1] and shape["row"] == shape["col"] == 4
        square = square and layers == 2
        if square and len(slab_widths(share, SLAB_PARTS)) == len(SLAB_PARTS):
            return gather_line(left_matrix, right_matrix)
        return gather_chain(left_matrix, right_matrix)

    step = jax.shard_map(local, mesh=mesh, in_specs=in_specs, out_specs=out_specs, check_vma=False)
    if shape["row"] == shape["col"] == 4 and shape["layer"] == 2:
        return step
    return step
```
